32 devices in a mesh: space: 16 (over z, y, core), tm: 2 (over x).
Axes of the slice: x: 2, y: 2, z: 4, core: 2. Of those that a mesh axis runs over, the one named last changes fastest.
Arguments:
- solutions: bfloat16 [2, 12, 8192, 128], P('tm', None, 'space'), may hold values from -6 to 6
- noise: int32 [2, 64, 12, 8192], P('tm', None, None, 'space'), may hold values from 0 to 3
- momenta: int32 [27, 3], replicated, may hold values from -2 to 2
- pairs: int32 [16, 2], P('tm'), may hold values from 0 to 1
Outputs:
- mesons: float32 [2, 2, 27, 64, 64], P('tm', None, None, 'space')
- correlators: float32 [16, 2, 27], P('tm')
The draws below stay inside these ranges and needn't reach their ends.
All inputs are finite; a program needn't handle non-finite values.
Results may differ from the reference program's by a relative error of at most 0.002.
Values sent between devices are 32-bit elements; how exact they have to be, the bound alone decides.
A program may use at most 64 MiB of HBM per device.

```python
import math
import jax
import jax.numpy as jnp
from jax import lax

NVEC = 64
SPINCOL = 12
MOMS = 27
EXTENT = 48
SITES = 8192
TSL = 2
NPAIRS = 16


def plant(drawn, rng, least, top_value):
    place = [jax.random.randint(jax.random.fold_in(rng, axis), (), 0, length) for axis, length in enumerate(drawn.shape)]
    main_axis = drawn.shape.index(max(drawn.shape))
    next_to = place[:main_axis] + [(place[main_axis] + 1) % drawn.shape[main_axis]] + place[main_axis + 1:]
    return drawn.at[tuple(place)].set(least).at[tuple(next_to)].set(top_value)


def level_of(key, extent, cuts, least, top_value):
    gain, own = 1.0, jax.random.fold_in(key, 6)
    for dim, parts in cuts:
        draws = jnp.exp(jax.random.uniform(jax.random.fold_in(own, dim), (parts,), jnp.float32, least / len(cuts), top_value / len(cuts)))
        gain = gain * jnp.repeat(draws, extent[dim] // parts).reshape([-1 if axis == dim else 1 for axis in range(len(extent))])
    return gain


def bell_draw(key, dims, scale, reach, split=(), held_as=jnp.bfloat16):
    result = jax.random.normal(key, dims, jnp.float32) * scale
    if len(split) > 0:
        result = level_of(key, dims, split, -0.22, 0.18) * result
    return jnp.clip(result, min=-reach, max=reach).astype(held_as)


def setup_inputs(seed: int = 0) -> dict:
    splits = jax.random.split(jax.random.key(seed), 5)
    return {
        "solutions": bell_draw(splits[0], (TSL, SPINCOL, SITES, 2 * NVEC), 1.0, 6.0, ((0, 2), (2, 16))),
        "noise": plant(jax.random.randint(splits[1], (TSL, NVEC, SPINCOL, SITES), 0, 4), jax.random.fold_in(splits[1], 1), 0, 3).astype(jnp.int32),
        "momenta": plant(jax.random.randint(splits[2], (MOMS, 3), -2, 3), jax.random.fold_in(splits[2], 1), -2, 2).astype(jnp.int32),
        "pairs": plant(jax.random.randint(splits[3], (NPAIRS, 2), 0, TSL), jax.random.fold_in(splits[3], 1), 0, TSL - 1).astype(jnp.int32),
    }


def phase_weights(noise_block, momenta, coords):
    qdotx = momenta[:, 0:1] * coords[0][None, :] + momenta[:, 1:2] * coords[1][None, :] + momenta[:, 2:3] * coords[2][None, :]
    index = (EXTENT // 4 * noise_block[None, :, :, :] + qdotx[:, None, None, :]) % EXTENT
    angle = index.astype(jnp.float32) * jnp.float32(2.0 * math.pi / EXTENT)
    rows = momenta.shape[0] * noise_block.shape[0]
    cols = noise_block.shape[1] * noise_block.shape[2]
    weight_re = jnp.cos(angle).astype(jnp.bfloat16).reshape(rows, cols)
    weight_im = (-jnp.sin(angle)).astype(jnp.bfloat16).reshape(rows, cols)
    return (weight_re, weight_im)

def site_coords(first, count):
    glob = first + jnp.arange(count, dtype=jnp.int32)
    return (glob % EXTENT, glob // EXTENT % EXTENT, glob // (EXTENT * EXTENT))

def slice_field(vectors, sources, momenta):
    block = min(1024, SITES)
    nblocks = SITES // block

    def one_block(step, total):
        first = (step * block).astype(jnp.int32)
        noise_block = lax.dynamic_slice_in_dim(sources, first, block, 2)
        vec_block = lax.dynamic_slice_in_dim(vectors, first, block, 1)
        weight_re, weight_im = phase_weights(noise_block, momenta, site_coords(first, block))
        stacked = vec_block.reshape(SPINCOL * block, 2 * NVEC)
        left = jnp.dot(weight_re, stacked, preferred_element_type=jnp.float32)
        right = jnp.dot(weight_im, stacked, preferred_element_type=jnp.float32)
        real_part = left[:, :NVEC] - right[:, NVEC:]
        imag_part = left[:, NVEC:] + right[:, :NVEC]
        return total + jnp.stack([real_part, imag_part], 0)
    start = jnp.zeros((2, MOMS * NVEC, NVEC), jnp.float32)
    total = lax.fori_loop(0, nblocks, one_block, start)
    return total.reshape(2, MOMS, NVEC, NVEC)

def reference(solutions, noise, momenta, pairs):
    scale = 1.0 / math.sqrt(SPINCOL * SITES)
    fields = [slice_field(solutions[t], noise[t], momenta) * scale for t in range(TSL)]
    mesons = jnp.stack(fields, 0)
    sink = mesons[pairs[:, 1]]
    source = mesons[pairs[:, 0]]
    real_part = lax.optimization_barrier(jnp.sum(sink[:, 0] * source[:, 0] + sink[:, 1] * source[:, 1], axis=(2, 3)))
    imag_part = lax.optimization_barrier(jnp.sum(sink[:, 1] * source[:, 0] - sink[:, 0] * source[:, 1], axis=(2, 3)))
    correlators = jnp.stack([real_part, imag_part], 1) / NVEC
    return (mesons, correlators)
```

```python
import functools
import math

import jax
import jax.numpy as jnp
from jax import lax
from jax.experimental import pallas as pl
from jax.experimental.pallas import tpu as pltpu
from jax.sharding import PartitionSpec as P

EXTENT = 48
QC = 4
MESH = pl.DeviceIdType.MESH


def phases(momenta, offset, sites, rows):
    glob = offset + jnp.arange(sites, dtype=jnp.int32)
    coords = (glob % EXTENT, glob // EXTENT % EXTENT, glob // (EXTENT * EXTENT))
    qdotx = (
        momenta[:, 0:1] * coords[0][None, :]
        + momenta[:, 1:2] * coords[1][None, :]
        + momenta[:, 2:3] * coords[2][None, :]
    )
    angle = (qdotx % EXTENT).astype(jnp.float32) * jnp.float32(2.0 * math.pi / EXTENT)
    base_re = jnp.cos(angle).astype(jnp.bfloat16)
    base_im = (-jnp.sin(angle)).astype(jnp.bfloat16)
    both = jnp.stack([base_re, base_im], 0).astype(jnp.float32)
    return jnp.pad(both, ((0, 0), (0, rows - momenta.shape[0]), (0, 0)))


def kernel(dims, base_ref, noise_hbm, sol_hbm, mes_ref, tr_ref,
           raw, sol, nre, nim, acc, sbuf, hbuf, qbuf, rcore, ry, rz, xb, ps,
           in_sem, cs, cr, ys, yr, zs, zr, xs, xr, pss, psr):
    nspace, nslices, nchunks, rows, nvec, spincol, scale = dims
    nz = nspace // 4
    me = lax.axis_index("space")
    slice_id = lax.axis_index("tm")
    core = lax.rem(me, 2)
    yy = lax.rem(me // 2, 2)
    zz = me // 4

    barrier = pltpu.get_barrier_semaphore()
    for o in range(1, nspace):
        pl.semaphore_signal(barrier, inc=1, device_id={"space": lax.rem(me + o, nspace)}, device_id_type=MESH)
    for o in range(1, nslices):
        pl.semaphore_signal(barrier, inc=1, device_id={"tm": lax.rem(slice_id + o, nslices)}, device_id_type=MESH)

    noise_copy = pltpu.make_async_copy(noise_hbm, raw, in_sem.at[0])
    sol_copy = pltpu.make_async_copy(sol_hbm, sol, in_sem.at[1])
    noise_copy.start()
    sol_copy.start()
    noise_copy.wait()

    def turn(a, carry):
        k = raw[:, a, :]
        one = jnp.float32(1.0)
        zero = jnp.float32(0.0)
        re = jnp.where(k == 0, one, jnp.where(k == 2, -one, zero))
        im = jnp.where(k == 3, one, jnp.where(k == 1, -one, zero))
        nre[a] = re.astype(jnp.bfloat16)
        nim[a] = im.astype(jnp.bfloat16)
        return carry

    for a in range(spincol):
        turn(a, 0)
    sol_copy.wait()

    lane = lax.broadcasted_iota(jnp.int32, (QC * nvec, 2 * nvec), 1)
    sign = jnp.where(lane < nvec, jnp.float32(-1.0), jnp.float32(1.0))
    lane_r = lax.broadcasted_iota(jnp.int32, (nchunks * QC * rows, 2 * nvec), 1)
    sign_r = jnp.where(lane_r < nvec, jnp.float32(-1.0), jnp.float32(1.0))

    def compute(c):
        acc[...] = jnp.zeros_like(acc)
        sites = base_ref.shape[2]

        def body(a, carry):
            wre, wim = [], []
            n_r, n_i = nre[a], nim[a]
            for qq in range(QC):
                q = c * QC + qq
                br = jnp.broadcast_to(base_ref[0, pl.ds(q, 1), :], (nvec, sites)).astype(jnp.bfloat16)
                bi = jnp.broadcast_to(base_ref[1, pl.ds(q, 1), :], (nvec, sites)).astype(jnp.bfloat16)
                wre.append(n_r * br - n_i * bi)
                wim.append(n_r * bi + n_i * br)
            w = jnp.concatenate(wre + wim, axis=0)
            acc[...] += jnp.dot(w, sol[a], preferred_element_type=jnp.float32)
            return carry

        lax.fori_loop(0, spincol, body, 0)
        left = acc[: QC * nvec, :]
        right = acc[QC * nvec:, :]
        field = left + pltpu.roll(right, nvec, 1) * sign
        for qq in range(QC):
            for d in range(nspace):
                first = qq * nvec + d * rows
                sbuf[c, d % 2, (d // 2) % 2, d // 4, qq * rows:(qq + 1) * rows, :] = field[first:first + rows, :]

    def remote(src, dst, ssem, rsem, where):
        return pltpu.make_async_remote_copy(src_ref=src, dst_ref=dst, send_sem=ssem, recv_sem=rsem,
                                            device_id=where, device_id_type=MESH)

    core_peer = {"space": me + 1 - 2 * core}
    y_peer = {"space": me + 2 - 4 * yy}

    def core_copy(c):
        return remote(sbuf.at[c, 1 - core], rcore.at[c], cs.at[c], cr.at[c], core_peer)

    def y_copy(c):
        return remote(hbuf.at[c, 1 - yy], ry.at[c], ys.at[c], yr.at[c], y_peer)

    def z_copy(c, o):
        to = lax.rem(zz + o, nz)
        return remote(qbuf.at[c, to], rz.at[c, o - 1], zs.at[c, o - 1], zr.at[c, o - 1],
                      {"space": to * 4 + yy * 2 + core})

    def x_copy(c, o):
        return remote(xb.at[slice_id, c], xb.at[slice_id, c], xs.at[c, o - 1], xr.at[c, o - 1],
                      {"tm": lax.rem(slice_id + o, nslices)})

    def p_copy(o):
        return remote(ps.at[me], ps.at[me], pss.at[o - 1], psr.at[o - 1],
                      {"space": lax.rem(me + o, nspace)})

    for step in range(nchunks + 3):
        c = step
        if c < nchunks:
            compute(c)
            if c == 0:
                pl.semaphore_wait(barrier, nspace - 1 + nslices - 1)
            core_copy(c).start()
        c = step - 1
        if 0 <= c < nchunks:
            core_copy(c).wait_recv()
            hbuf[c, 1 - yy] = sbuf[c, core, 1 - yy] + rcore[c, 1 - yy]
            y_copy(c).start()
            hbuf[c, yy] = sbuf[c, core, yy] + rcore[c, yy]
        c = step - 2
        if 0 <= c < nchunks:
            y_copy(c).wait_recv()
            qbuf[c] = hbuf[c, yy] + ry[c]
            for o in range(1, nz):
                z_copy(c, o).start()
        c = step - 3
        if 0 <= c < nchunks:
            for o in range(1, nz):
                z_copy(c, o).wait_recv()
            total = qbuf[c, zz]
            for o in range(1, nz):
                total = total + rz[c, o - 1]
            total = total * jnp.float32(scale)
            xb[slice_id, c] = total
            mes_ref[c] = total
            for o in range(1, nslices):
                x_copy(c, o).start()

    for c in range(nchunks):
        for o in range(1, nslices):
            x_copy(c, o).wait_recv()

    lq = nchunks * QC * rows
    trows = ps.shape[1]
    rowid = lax.broadcasted_iota(jnp.int32, (trows, 2 * nvec), 0)
    found = jnp.zeros((trows, lq), jnp.float32)

    def add(found, row, prod):
        pick = jnp.where(rowid == row, jnp.float32(1.0), jnp.float32(0.0))
        return found + lax.dot_general(pick, prod, (((1,), (1,)), ((), ())), precision=lax.Precision.HIGHEST,
                                       preferred_element_type=jnp.float32)

    for w in range(nslices):
        mw = xb[w].reshape(lq, 2 * nvec)
        for u in range(w + 1):
            mu = xb[u].reshape(lq, 2 * nvec)
            found = add(found, w * nslices + u, mw * mu)
            if u < w:
                found = add(found, u * nslices + w, mw * (pltpu.roll(mu, nvec, 1) * sign_r))
    ps[me] = jnp.zeros(ps.shape[1:], jnp.float32)
    ps[me, :, :lq] = found
    for o in range(1, nspace):
        p_copy(o).start()
    for o in range(1, nspace):
        p_copy(o).wait_recv()
    total = ps[0]
    for d in range(1, nspace):
        total = total + ps[d]
    tr_ref[...] = total

    for c in range(nchunks):
        core_copy(c).wait_send()
        y_copy(c).wait_send()
        for o in range(1, nz):
            z_copy(c, o).wait_send()
        for o in range(1, nslices):
            x_copy(c, o).wait_send()
    for o in range(1, nspace):
        p_copy(o).wait_send()


def local(solutions, noise, momenta, pairs):
    _, spincol, sites, width = solutions.shape
    nvec = width // 2
    moms = momenta.shape[0]
    nspace = lax.axis_size("space")
    nslices = lax.axis_size("tm")
    nz = nspace // 4
    rows = nvec // nspace
    nchunks = -(-moms // QC)
    scale = 1.0 / math.sqrt(spincol * sites * nspace)
    offset = lax.axis_index("space") * sites
    base = phases(momenta, offset, sites, -(-nchunks * QC // 8) * 8)
    trows = -(-nslices * nslices // 8) * 8
    lq = nchunks * QC * rows
    lpad = -(-lq // 128) * 128
    dims = (nspace, nslices, nchunks, rows, nvec, spincol, scale)
    f32 = jnp.float32
    blk = (QC * rows, width)
    dma = pltpu.SemaphoreType.DMA
    vmem = pl.BlockSpec(memory_space=pltpu.VMEM)
    hbm = pl.BlockSpec(memory_space=pl.ANY)
    mes, traces = pl.pallas_call(
        functools.partial(kernel, dims),
        out_shape=(jax.ShapeDtypeStruct((nchunks,) + blk, f32), jax.ShapeDtypeStruct((trows, lpad), f32)),
        in_specs=[vmem, hbm, hbm],
        out_specs=(vmem, vmem),
        scratch_shapes=[
            pltpu.VMEM((nvec, spincol, sites), jnp.int32),
            pltpu.VMEM((spincol, sites, width), jnp.bfloat16),
            pltpu.VMEM((spincol, nvec, sites), jnp.bfloat16),
            pltpu.VMEM((spincol, nvec, sites), jnp.bfloat16),
            pltpu.VMEM((2 * QC * nvec, width), f32),
            pltpu.VMEM((nchunks, 2, 2, nz) + blk, f32),
            pltpu.VMEM((nchunks, 2, nz) + blk, f32),
            pltpu.VMEM((nchunks, nz) + blk, f32),
            pltpu.VMEM((nchunks, 2, nz) + blk, f32),
            pltpu.VMEM((nchunks, nz) + blk, f32),
            pltpu.VMEM((nchunks, nz - 1) + blk, f32),
            pltpu.VMEM((nslices, nchunks) + blk, f32),
            pltpu.VMEM((nspace, trows, lpad), f32),
            dma((2,)),
            dma((nchunks,)), dma((nchunks,)),
            dma((nchunks,)), dma((nchunks,)),
            dma((nchunks, nz - 1)), dma((nchunks, nz - 1)),
            dma((nchunks, nslices - 1)), dma((nchunks, nslices - 1)),
            dma((nspace - 1,)), dma((nspace - 1,)),
        ],
        compiler_params=pltpu.CompilerParams(collective_id=0, has_side_effects=True, vmem_limit_bytes=60 * 2**20),
    )(base, noise[0], solutions[0])
    mesons = mes.reshape(nchunks * QC, rows, 2, nvec)[:moms].transpose(2, 0, 1, 3)[None]
    table = jnp.sum(traces[:, :lq].reshape(trows, nchunks * QC, rows), axis=2)[:, :moms] / nvec
    source, sink = pairs[:, 0], pairs[:, 1]
    high, low = jnp.maximum(source, sink), jnp.minimum(source, sink)
    slots = jnp.arange(trows, dtype=jnp.int32)

    def pick(index):
        return jnp.sum(jnp.where((index[:, None] == slots[None, :])[:, :, None], table[None], 0.0), axis=1)

    real = pick(high * nslices + low)
    imag = pick(low * nslices + high)
    imag = jnp.where((sink > source)[:, None], imag, jnp.where((sink < source)[:, None], -imag, 0.0))
    return (mesons, jnp.stack([real, imag], 1))


def solution(mesh):
    in_specs = (P("tm", None, "space", None), P("tm", None, None, "space"), P(), P("tm", None))
    out_specs = (P("tm", None, None, "space", None), P("tm", None, None))
    return jax.shard_map(local, mesh=mesh, in_specs=in_specs, out_specs=out_specs, check_vma=False)
```

```python
import functools
import math

import jax
import jax.numpy as jnp
from jax import lax
from jax.experimental import pallas as pl
from jax.experimental.pallas import tpu as pltpu
from jax.sharding import PartitionSpec as P

EXTENT = 48
QC = 4
GROUP = 2
MESH = pl.DeviceIdType.MESH


def wrap(value):
    return jnp.floor((value + 0.5) * jnp.float32(1.0 / EXTENT))


def column(ref, row):
    size = ref.shape[1]
    here = lax.broadcasted_iota(jnp.int32, (size, size), 0)
    there = lax.broadcasted_iota(jnp.int32, (size, size), 1)
    line = jnp.broadcast_to(ref[row:row + 1, :].astype(jnp.float32), (size, size))
    return jnp.sum(jnp.where(here == there, line, jnp.float32(0.0)), axis=1, keepdims=True)


def phases(mom_ref, offset, sites):
    moms = mom_ref.shape[1]
    glob = (lax.broadcasted_iota(jnp.int32, (moms, sites), 1) + offset).astype(jnp.float32)
    line = wrap(glob)
    plane = wrap(line)
    xx = glob - line * EXTENT
    yy = line - plane * EXTENT
    dot = column(mom_ref, 0) * xx + column(mom_ref, 1) * yy + column(mom_ref, 2) * plane
    angle = (dot - wrap(dot) * EXTENT) * jnp.float32(2.0 * math.pi / EXTENT)
    base_re = jnp.cos(angle).astype(jnp.bfloat16).astype(jnp.float32)
    base_im = (-jnp.sin(angle)).astype(jnp.bfloat16).astype(jnp.float32)
    return base_re, base_im


def kernel(dims, mom_ref, pair_ref, noise_hbm, sol_hbm, mes_ref, tr_ref,
           base_ref, raw, sol, nre, nim, acc, sbuf, hbuf, qbuf, rcore, ry, rz, xb, ps,
           in_sem, cs, cr, ys, yr, zs, zr, xs, xr, pss, psr):
    nspace, nslices, nchunks, rows, nvec, spincol, scale = dims
    nz = nspace // 4
    me = lax.axis_index("space")
    slice_id = lax.axis_index("tm")
    core = lax.rem(me, 2)
    yy = lax.rem(me // 2, 2)
    zz = me // 4

    barrier = pltpu.get_barrier_semaphore()
    for o in range(1, nspace):
        pl.semaphore_signal(barrier, inc=1, device_id={"space": lax.rem(me + o, nspace)}, device_id_type=MESH)
    for o in range(1, nslices):
        pl.semaphore_signal(barrier, inc=1, device_id={"tm": lax.rem(slice_id + o, nslices)}, device_id_type=MESH)

    noise_copy = pltpu.make_async_copy(noise_hbm, raw, in_sem.at[0])
    sol_copy = pltpu.make_async_copy(sol_hbm, sol, in_sem.at[1])
    noise_copy.start()
    sol_copy.start()
    moms = mom_ref.shape[1]
    base_re, base_im = phases(mom_ref, me * sol.shape[1], sol.shape[1])
    base_ref[...] = jnp.zeros_like(base_ref)
    base_ref[0, :moms] = base_re
    base_ref[1, :moms] = base_im
    noise_copy.wait()

    def turn(a, carry):
        k = raw[a]
        one = jnp.float32(1.0)
        zero = jnp.float32(0.0)
        re = jnp.where(k == 0, one, jnp.where(k == 2, -one, zero))
        im = jnp.where(k == 3, one, jnp.where(k == 1, -one, zero))
        nre[a] = re.astype(jnp.bfloat16)
        nim[a] = im.astype(jnp.bfloat16)
        return carry

    for a in range(spincol):
        turn(a, 0)
    sol_copy.wait()

    lane = lax.broadcasted_iota(jnp.int32, (QC * nvec, 2 * nvec), 1)
    sign = jnp.where(lane < nvec, jnp.float32(-1.0), jnp.float32(1.0))
    lane_r = lax.broadcasted_iota(jnp.int32, (nchunks * QC * rows, 2 * nvec), 1)
    sign_r = jnp.where(lane_r < nvec, jnp.float32(-1.0), jnp.float32(1.0))

    def compute(c):
        acc[...] = jnp.zeros_like(acc)
        sites = base_ref.shape[2]

        def body(step, carry):
            columns = []
            for k in range(GROUP):
                a = step * GROUP + k
                wre, wim = [], []
                n_r, n_i = nre[a], nim[a]
                for qq in range(QC):
                    q = c * QC + qq
                    br = jnp.broadcast_to(base_ref[0, pl.ds(q, 1), :].astype(jnp.bfloat16), (nvec, sites))
                    bi = jnp.broadcast_to(base_ref[1, pl.ds(q, 1), :].astype(jnp.bfloat16), (nvec, sites))
                    wre.append(n_r * br - n_i * bi)
                    wim.append(n_r * bi + n_i * br)
                columns.append(jnp.concatenate(wre + wim, axis=0))
            w = jnp.concatenate(columns, axis=1)
            v = sol[pl.ds(step * GROUP, GROUP)].reshape(GROUP * sites, 2 * nvec)
            acc[...] += jnp.dot(w, v, preferred_element_type=jnp.float32)
            return carry

        lax.fori_loop(0, spincol // GROUP, body, 0)
        left = acc[: QC * nvec, :]
        right = acc[QC * nvec:, :]
        field = left + pltpu.roll(right, nvec, 1) * sign
        for qq in range(QC):
            for d in range(nspace):
                first = qq * nvec + d * rows
                sbuf[c, d % 2, (d // 2) % 2, d // 4, qq * rows:(qq + 1) * rows, :] = field[first:first + rows, :]

    def remote(src, dst, ssem, rsem, where):
        return pltpu.make_async_remote_copy(src_ref=src, dst_ref=dst, send_sem=ssem, recv_sem=rsem,
                                            device_id=where, device_id_type=MESH)

    core_peer = {"space": me + 1 - 2 * core}
    y_peer = {"space": me + 2 - 4 * yy}

    def core_copy(c):
        return remote(sbuf.at[c, 1 - core], rcore.at[c], cs.at[c], cr.at[c], core_peer)

    def y_copy(c):
        return remote(hbuf.at[c, 1 - yy], ry.at[c], ys.at[c], yr.at[c], y_peer)

    def z_copy(c, o):
        to = lax.rem(zz + o, nz)
        return remote(qbuf.at[c, to], rz.at[c, o - 1], zs.at[c, o - 1], zr.at[c, o - 1],
                      {"space": to * 4 + yy * 2 + core})

    def x_copy(c, o):
        return remote(xb.at[slice_id, c], xb.at[slice_id, c], xs.at[c, o - 1], xr.at[c, o - 1],
                      {"tm": lax.rem(slice_id + o, nslices)})

    def p_copy(o):
        return remote(ps.at[me], ps.at[me], pss.at[o - 1], psr.at[o - 1],
                      {"space": lax.rem(me + o, nspace)})

    for step in range(nchunks + 3):
        c = step
        if c < nchunks:
            compute(c)
            if c == 0:
                pl.semaphore_wait(barrier, nspace - 1 + nslices - 1)
            core_copy(c).start()
        c = step - 1
        if 0 <= c < nchunks:
            core_copy(c).wait_recv()
            hbuf[c, 1 - yy] = sbuf[c, core, 1 - yy] + rcore[c, 1 - yy]
            y_copy(c).start()
            hbuf[c, yy] = sbuf[c, core, yy] + rcore[c, yy]
        c = step - 2
        if 0 <= c < nchunks:
            y_copy(c).wait_recv()
            qbuf[c] = hbuf[c, yy] + ry[c]
            for o in range(1, nz):
                z_copy(c, o).start()
        c = step - 3
        if 0 <= c < nchunks:
            for o in range(1, nz):
                z_copy(c, o).wait_recv()
            total = qbuf[c, zz]
            for o in range(1, nz):
                total = total + rz[c, o - 1]
            total = total * jnp.float32(scale)
            xb[slice_id, c] = total
            for qq in range(min(QC, moms - c * QC)):
                part = total[qq * rows:(qq + 1) * rows, :]
                mes_ref[0, c * QC + qq] = part[:, :nvec]
                mes_ref[1, c * QC + qq] = part[:, nvec:]
            for o in range(1, nslices):
                x_copy(c, o).start()

    for c in range(nchunks):
        for o in range(1, nslices):
            x_copy(c, o).wait_recv()

    lq = nchunks * QC * rows
    trows = ps.shape[1]
    rowid = lax.broadcasted_iota(jnp.int32, (trows, 2 * nvec), 0)
    found = jnp.zeros((trows, lq), jnp.float32)

    def add(found, row, prod):
        pick = jnp.where(rowid == row, jnp.float32(1.0), jnp.float32(0.0))
        return found + lax.dot_general(pick, prod, (((1,), (1,)), ((), ())), precision=lax.Precision.HIGHEST,
                                       preferred_element_type=jnp.float32)

    for w in range(nslices):
        mw = xb[w].reshape(lq, 2 * nvec)
        for u in range(w + 1):
            mu = xb[u].reshape(lq, 2 * nvec)
            found = add(found, w * nslices + u, mw * mu)
            if u < w:
                found = add(found, u * nslices + w, mw * (pltpu.roll(mu, nvec, 1) * sign_r))
    ps[me] = jnp.zeros(ps.shape[1:], jnp.float32)
    ps[me, :, :lq] = found
    for o in range(1, nspace):
        p_copy(o).start()
    for o in range(1, nspace):
        p_copy(o).wait_recv()
    total = ps[0]
    for d in range(1, nspace):
        total = total + ps[d]
    lpad = total.shape[1]
    left_id = lax.broadcasted_iota(jnp.int32, (lpad, 128), 0)
    first = lax.broadcasted_iota(jnp.int32, (lpad, 128), 1) * rows
    fold = jnp.where((left_id >= first) & (left_id < first + rows), jnp.float32(1.0), jnp.float32(0.0))

    def exact_dot(p, r):
        return jnp.dot(p, r, precision=lax.Precision.HIGHEST, preferred_element_type=jnp.float32)

    table = exact_dot(total, fold) * jnp.float32(1.0 / nvec)
    source, sink = column(pair_ref, 0).astype(jnp.int32), column(pair_ref, 1).astype(jnp.int32)
    high, low = jnp.maximum(source, sink), jnp.minimum(source, sink)
    slot = lax.broadcasted_iota(jnp.int32, (pair_ref.shape[1], trows), 1)
    one, zero = jnp.float32(1.0), jnp.float32(0.0)
    turned = jnp.where(sink > source, one, jnp.where(sink < source, -one, zero))
    real = exact_dot(jnp.where(slot == high * nslices + low, one, zero), table)
    imag = exact_dot(jnp.where(slot == low * nslices + high, turned, zero), table)
    tr_ref[:, 0, :] = real[:, :moms]
    tr_ref[:, 1, :] = imag[:, :moms]

    for c in range(nchunks):
        core_copy(c).wait_send()
        y_copy(c).wait_send()
        for o in range(1, nz):
            z_copy(c, o).wait_send()
        for o in range(1, nslices):
            x_copy(c, o).wait_send()
    for o in range(1, nspace):
        p_copy(o).wait_send()


def local(solutions, noise, momenta, pairs):
    _, spincol, sites, width = solutions.shape
    nvec = width // 2
    moms = momenta.shape[0]
    nspace = lax.axis_size("space")
    nslices = lax.axis_size("tm")
    nz = nspace // 4
    rows = nvec // nspace
    nchunks = -(-moms // QC)
    scale = 1.0 / math.sqrt(spincol * sites * nspace)
    trows = -(-nslices * nslices // 8) * 8
    lq = nchunks * QC * rows
    lpad = -(-lq // 128) * 128
    dims = (nspace, nslices, nchunks, rows, nvec, spincol, scale)
    f32 = jnp.float32
    blk = (QC * rows, width)
    dma = pltpu.SemaphoreType.DMA
    vmem = pl.BlockSpec(memory_space=pltpu.VMEM)
    hbm = pl.BlockSpec(memory_space=pl.ANY)
    mesons, correlators = pl.pallas_call(
        functools.partial(kernel, dims),
        out_shape=(jax.ShapeDtypeStruct((2, moms, rows, nvec), f32),
                   jax.ShapeDtypeStruct((pairs.shape[0], 2, moms), f32)),
        in_specs=[vmem, vmem, hbm, hbm],
        out_specs=(vmem, vmem),
        scratch_shapes=[
            pltpu.VMEM((2, -(-nchunks * QC // 8) * 8, sites), f32),
            pltpu.VMEM((spincol, nvec, sites), jnp.int32),
            pltpu.VMEM((spincol, sites, width), jnp.bfloat16),
            pltpu.VMEM((spincol, nvec, sites), jnp.bfloat16),
            pltpu.VMEM((spincol, nvec, sites), jnp.bfloat16),
            pltpu.VMEM((2 * QC * nvec, width), f32),
            pltpu.VMEM((nchunks, 2, 2, nz) + blk, f32),
            pltpu.VMEM((nchunks, 2, nz) + blk, f32),
            pltpu.VMEM((nchunks, nz) + blk, f32),
            pltpu.VMEM((nchunks, 2, nz) + blk, f32),
            pltpu.VMEM((nchunks, nz) + blk, f32),
            pltpu.VMEM((nchunks, nz - 1) + blk, f32),
            pltpu.VMEM((nslices, nchunks) + blk, f32),
            pltpu.VMEM((nspace, trows, lpad), f32),
            dma((2,)),
            dma((nchunks,)), dma((nchunks,)),
            dma((nchunks,)), dma((nchunks,)),
            dma((nchunks, nz - 1)), dma((nchunks, nz - 1)),
            dma((nchunks, nslices - 1)), dma((nchunks, nslices - 1)),
            dma((nspace - 1,)), dma((nspace - 1,)),
        ],
        compiler_params=pltpu.CompilerParams(collective_id=0, has_side_effects=True, vmem_limit_bytes=60 * 2**20),
    )(momenta.T, pairs.T, noise[0].transpose(1, 0, 2), solutions[0])
    return (mesons[None], correlators)


def solution(mesh):
    in_specs = (P("tm", None, "space", None), P("tm", None, None, "space"), P(), P("tm", None))
    out_specs = (P("tm", None, None, "space", None), P("tm", None, None))
    return jax.shard_map(local, mesh=mesh, in_specs=in_specs, out_specs=out_specs, check_vma=False)
```
